32 devices in a mesh: graph: 16 (over z, y, core), chan: 2 (over x).
Axes of the slice: x: 2, y: 2, z: 4, core: 2. Of those that a mesh axis runs over, the one named last changes fastest.
Arguments:
- embed: bfloat16 [25, 512, 2048], P(None, 'chan', 'graph'), may hold values from -200 to 200
- gain: float32 [5, 512], P(None, 'chan'), may hold values from 0.25 to 1.75
- w_zero: bfloat16 [5, 512, 2560], P(None, 'chan'), may hold values from -0.125 to 0.125
- w_one: bfloat16 [2, 4, 512, 2048], P(None, None, 'chan'), may hold values from -0.125 to 0.125
- w_two: bfloat16 [2, 3, 512, 1536], P(None, None, 'chan'), may hold values from -0.15625 to 0.15625
- rot_table: float32 [19, 25, 256], replicated, may hold values from -1 to 1, as said below
- face_atoms: int32 [512], P('graph'), may hold values from 0 to 127, as said below
- edge_source: int32 [2048], P('graph'), may hold values from 0 to 159
- edge_target: int32 [2048], P('graph'), may hold values from 0 to 127
- rot_index: int32 [2048], P('graph'), may hold values from 0 to 255
- edge_weight: float32 [2048], P('graph'), may hold values from 0.2 to 1
- cotangent: bfloat16 [25, 512, 2048], P(None, 'chan', 'graph'), may hold values from -1.5 to 1.5
Outputs:
- update: bfloat16 [25, 512, 2048], P(None, 'chan', 'graph')
- grad_embed: bfloat16 [25, 512, 2048], P(None, 'chan', 'graph')
- grad_zero: float32 [5, 512, 2560], P(None, 'chan', 'graph')
- grad_one: float32 [2, 4, 512, 2048], P(None, None, 'chan', 'graph')
- grad_two: float32 [2, 3, 512, 1536], P(None, None, 'chan', 'graph')
The draws below stay inside these ranges and needn't reach their ends.
Inputs may be any that keep to these rules, and one draw needn't show every extreme that they name: `rot_table`: for every rotation, frame row (m, l) is nonzero only on the 2l + 1 coefficients of degree l, where it is row l + m of an orthogonal (2l + 1)-square matrix shared by the rows of that degree; the degree-0 entry is 1. `face_atoms`: block b holds 32 distinct atom indices counted from the first atom of block b: the first 16 lie at the face toward block b - 1, the last 16 at the face toward block b + 1. `edge_source`: read as in the step that defines src. `edge_target`: counted from the first atom of the edge's block.
All inputs are finite; a program needn't handle non-finite values.
Results may differ from the reference program's by a relative error of at most 0.0062.
Values may be sent and summed in bfloat16 or wider, within the bound.
No kernel may reach another device: no remote copies, remote signals or barrier semaphores. Data moves between devices by JAX's collectives and lax.ppermute only.
A program may use at most 192 MiB of HBM per device.

```python
import math
import jax
import jax.numpy as jnp
from jax import lax

C = 512
ATOM_DEV = 128
HALO = 16
EDGE_DEV = 128
ROTS = 256
ATOMS = 2048
EDGES = 2048
FACES = 512
N_GRAPH = 16


FRAME = ((0, 0), (1, 0), (2, 0), (3, 0), (4, 0), (1, 1), (2, 1), (3, 1), (4, 1), (1, -1), (2, -1), (3, -1), (4, -1), (2, 2), (3, 2), (4, 2), (2, -2), (3, -2), (4, -2))


def draw_embed(key, part):
    keys = jax.random.split(key, 4)
    ramp = jnp.arange(C, dtype=jnp.float32) / C - 0.5
    channel_scale = jnp.exp(math.log(10.0) * ramp) * jax.random.uniform(keys[1], (C,), jnp.float32, 0.7, 1.4)
    atom_scale = jnp.exp(jax.random.uniform(keys[2], (ATOMS,), jnp.float32, math.log(0.3), math.log(3.0)))
    raw = jnp.clip(jax.random.normal(keys[0], (25, C, ATOMS), jnp.float32), -6.0, 6.0)
    values = raw * channel_scale[None, :, None] * atom_scale[None, None, :]
    return jnp.clip(values, -200.0, 200.0).astype(jnp.bfloat16)


def reflect_block(key, size):
    matrix = jnp.broadcast_to(jnp.eye(size, dtype=jnp.float32), (ROTS, size, size))
    for index in range(size):
        vector = jax.random.normal(jax.random.fold_in(key, index), (ROTS, size), jnp.float32)
        vector = vector / jnp.sqrt(jnp.sum(vector * vector, axis=1, keepdims=True) + 1e-12)
        folded = jnp.einsum('rj,rjk->rk', vector, matrix)
        matrix = matrix - 2.0 * vector[:, :, None] * folded[:, None, :]
    return matrix


def draw_rot_table(key, part):
    blocks = [jnp.ones((ROTS, 1, 1), jnp.float32)]
    for degree in range(1, 5):
        blocks.append(reflect_block(jax.random.fold_in(key, 100 + degree), 2 * degree + 1))
    lines = []
    for pair in FRAME:
        degree = pair[0]
        line = jnp.zeros((ROTS, 25), jnp.float32)
        line = line.at[:, degree * degree:(degree + 1) * (degree + 1)].set(blocks[degree][:, degree + pair[1], :])
        lines.append(line)
    table = jnp.stack(lines, axis=0)
    return jnp.transpose(table, (0, 2, 1))


def draw_face_atoms(key, part):
    count = FACES // (2 * HALO)
    keys = jax.random.split(key, count)
    picks = jax.vmap(lambda single: jax.random.permutation(single, ATOM_DEV)[:2 * HALO])(keys)
    return picks.reshape(FACES).astype(jnp.int32)


def with_ends(entries, own_key, low, largest):
    longest = entries.shape.index(max(entries.shape))
    spots = []
    for shift in (0, 1):
        where = [jax.random.randint(jax.random.fold_in(own_key, axis), (), 0, length) for axis, length in enumerate(entries.shape)]
        where[longest] = (where[longest] + shift) % entries.shape[longest]
        spots.append(tuple(where))
    return entries.at[spots[0]].set(low).at[spots[1]].set(largest)


def steps_of(own_key, extent, shards, low, high):
    def one(axis_at, blocks):
        heights = jax.random.uniform(jax.random.fold_in(jax.random.fold_in(own_key, 6), axis_at), (blocks,), jnp.float32, low / len(shards), high / len(shards))
        return jnp.repeat(jnp.exp(heights), extent[axis_at] // blocks).reshape((-1,) + (1,) * (len(extent) - axis_at - 1))

    factor_of = one(*shards[0])
    for cut in shards[1:]:
        factor_of = factor_of * one(*cut)
    return factor_of


def normal_values(rng, dims, scale, reach, cuts=(), kind=jnp.bfloat16):
    entries = scale * jax.random.normal(rng, dims, jnp.float32)
    if cuts:
        entries = entries * steps_of(rng, dims, cuts, -0.22, 0.18)
    return jnp.clip(entries, -reach, reach).astype(kind)


def setup_inputs(seed: int = 0) -> dict:
    splits = jax.random.split(jax.random.key(seed), 13)
    embed = draw_embed(jax.random.fold_in(splits[12], 71), 0)
    gain = jnp.clip(1.0 + 0.15 * jax.random.normal(splits[1], (5, C), jnp.float32), 0.25, 1.75)
    w_zero = normal_values(splits[2], (5, C, 5 * C), (5 * C) ** -0.5, 0.125, ((1, 2),))
    w_one = normal_values(splits[3], (2, 4, C, 4 * C), (4 * C) ** -0.5, 0.125, ((2, 2),))
    w_two = normal_values(splits[4], (2, 3, C, 3 * C), (3 * C) ** -0.5, 0.15625, ((2, 2),))
    rot_table = draw_rot_table(jax.random.fold_in(splits[12], 71), 0)
    face_atoms = draw_face_atoms(jax.random.fold_in(splits[12], 71), 0)
    edge_source = with_ends(jax.random.randint(splits[7], (EDGES,), 0, ATOM_DEV + 2 * HALO), jax.random.fold_in(splits[7], 1), 0, (ATOM_DEV + 2 * HALO) - 1).astype(jnp.int32)
    edge_target = with_ends(jax.random.randint(splits[8], (EDGES,), 0, ATOM_DEV), jax.random.fold_in(splits[8], 1), 0, ATOM_DEV - 1).astype(jnp.int32)
    rot_index = with_ends(jax.random.randint(splits[9], (EDGES,), 0, ROTS), jax.random.fold_in(splits[9], 1), 0, ROTS - 1).astype(jnp.int32)
    edge_weight = jnp.clip(jnp.exp(math.log(1.0) - 1.609438 * jax.random.uniform(splits[10], (EDGES,), jnp.float32) ** steps_of(splits[10], (EDGES,), ((0, 16),), -0.2, 0.2)), 0.2, 1.0)
    cotangent = normal_values(splits[11], (25, C, ATOMS), 0.25, 1.5, ((1, 2), (2, 16)))
    return {"embed": embed, "gain": gain, "w_zero": w_zero, "w_one": w_one, "w_two": w_two, "rot_table": rot_table, "face_atoms": face_atoms, "edge_source": edge_source, "edge_target": edge_target, "rot_index": rot_index, "edge_weight": edge_weight, "cotangent": cotangent}


EPSILON = 1e-06
HIGHEST = lax.Precision.HIGHEST
FRAME = ((0, 0), (1, 0), (2, 0), (3, 0), (4, 0), (1, 1), (2, 1), (3, 1), (4, 1), (1, -1), (2, -1), (3, -1), (4, -1), (2, 2), (3, 2), (4, 2), (2, -2), (3, -2), (4, -2))

def gain_rows(gain):
    pieces = [jnp.broadcast_to(gain[degree:degree + 1], (2 * degree + 1, gain.shape[1])) for degree in range(5)]
    return jnp.concatenate(pieces, axis=0)

def product(left, right):
    return jnp.dot(left, right, preferred_element_type=jnp.float32)

def across(left, right):
    return lax.dot_general(left, right, (((0,), (0,)), ((), ())), preferred_element_type=jnp.float32)

def outer(left, right):
    return lax.dot_general(left, right, (((1,), (1,)), ((), ())), preferred_element_type=jnp.float32)

def stack_frame(parts, width, edges):
    row_counts = (5, 4, 4, 3, 3)
    return jnp.concatenate([part.reshape(rows, width, edges) for part, rows in zip(parts, row_counts)], axis=0)

def mix_part(w_zero, w_one, w_two, piece, start):
    count = piece.shape[1]
    edges = piece.shape[2]
    outputs = w_zero.shape[1]

    def columns(weight, blocks):
        shaped = weight.reshape(blocks * outputs, blocks, weight.shape[-1] // blocks)
        return lax.dynamic_slice_in_dim(shaped, start, count, 2).reshape(blocks * outputs, blocks * count)

    def frame_rows(first, blocks):
        return piece[first:first + blocks].reshape(blocks * count, edges)
    parts = [product(columns(w_zero, 5), frame_rows(0, 5))]
    for weights, first, blocks in ((w_one, 5, 4), (w_two, 13, 3)):
        real_part = columns(weights[0], blocks)
        imag_part = columns(weights[1], blocks)
        plus = frame_rows(first, blocks)
        minus = frame_rows(first + blocks, blocks)
        parts.append(product(real_part, plus) - product(imag_part, minus))
        parts.append(product(real_part, minus) + product(imag_part, plus))
    return tuple(parts)

def mix_backward(w_zero, w_one, w_two, grads, frame):
    outputs = grads.shape[1]
    width = frame.shape[1]
    edges = grads.shape[2]

    def grad_rows(first, blocks):
        return grads[first:first + blocks].reshape(blocks * outputs, edges)

    def frame_rows(first, blocks):
        return frame[first:first + blocks].reshape(blocks * width, edges)
    zero_weight = w_zero.reshape(5 * outputs, 5 * width)
    grad_first = grad_rows(0, 5)
    back = [across(zero_weight, grad_first)]
    weight_zero = outer(grad_first, frame_rows(0, 5)).reshape(5, outputs, 5 * width)
    pairs = []
    for weights, first, blocks in ((w_one, 5, 4), (w_two, 13, 3)):
        real_part = weights[0].reshape(blocks * outputs, blocks * width)
        imag_part = weights[1].reshape(blocks * outputs, blocks * width)
        grad_plus = grad_rows(first, blocks)
        grad_minus = grad_rows(first + blocks, blocks)
        frame_plus = frame_rows(first, blocks)
        frame_minus = frame_rows(first + blocks, blocks)
        back.append(across(real_part, grad_plus) + across(imag_part, grad_minus))
        back.append(across(real_part, grad_minus) - across(imag_part, grad_plus))
        real_grad = outer(grad_plus, frame_plus) + outer(grad_minus, frame_minus)
        imag_grad = outer(grad_minus, frame_plus) - outer(grad_plus, frame_minus)
        pairs.append(jnp.stack([real_grad.reshape(blocks, outputs, blocks * width), imag_grad.reshape(blocks, outputs, blocks * width)]))
    return (stack_frame(back, width, edges), weight_zero, pairs[0], pairs[1])

def reference(embed, gain, w_zero, w_one, w_two, rot_table, face_atoms, edge_source, edge_target, rot_index, edge_weight, cotangent):
    values = embed.astype(jnp.float32)
    gains = gain_rows(gain)
    inverse = lax.rsqrt(lax.optimization_barrier(jnp.sum(values * values, axis=(0, 1))) / (25 * C) + EPSILON)
    normed = (values * inverse[None, None, :] * gains[:, :, None]).astype(jnp.bfloat16)
    positions = jnp.arange(ATOM_DEV, dtype=jnp.int32)

    def shard_step(carry, shard):
        update, grad_normed, grad_zero, grad_one, grad_two = carry
        left = (shard - 1) % N_GRAPH
        right = (shard + 1) % N_GRAPH
        from_left = lax.dynamic_slice_in_dim(face_atoms, left * (2 * HALO) + HALO, HALO)
        from_right = lax.dynamic_slice_in_dim(face_atoms, right * (2 * HALO), HALO)
        lookup = jnp.concatenate([shard * ATOM_DEV + positions, left * ATOM_DEV + from_left, right * ATOM_DEV + from_right]).astype(jnp.int32)
        first = (shard * EDGE_DEV).astype(jnp.int32)
        sources = lookup[lax.dynamic_slice_in_dim(edge_source, first, EDGE_DEV)]
        targets = (shard * ATOM_DEV + lax.dynamic_slice_in_dim(edge_target, first, EDGE_DEV)).astype(jnp.int32)
        rotations = jnp.take(rot_table, lax.dynamic_slice_in_dim(rot_index, first, EDGE_DEV), axis=2)
        scale = lax.dynamic_slice_in_dim(edge_weight, first, EDGE_DEV)
        gathered = jnp.take(normed, sources, axis=2).astype(jnp.float32)
        frame = jnp.einsum('jke,kce->jce', rotations, gathered, precision=HIGHEST).astype(jnp.bfloat16)
        mixed = stack_frame(mix_part(w_zero, w_one, w_two, frame, 0), C, EDGE_DEV)
        message = jnp.einsum('jke,jce->kce', rotations, mixed * scale[None, None, :], precision=HIGHEST).astype(jnp.bfloat16)
        update = update.at[:, :, targets].add(message.astype(jnp.float32))
        arriving = jnp.take(cotangent, targets, axis=2).astype(jnp.float32)
        grads = (jnp.einsum('jke,kce->jce', rotations, arriving, precision=HIGHEST) * scale[None, None, :]).astype(jnp.bfloat16)
        back, part_zero, part_one, part_two = mix_backward(w_zero, w_one, w_two, grads, frame)
        spread = jnp.einsum('jke,jce->kce', rotations, back, precision=HIGHEST)
        grad_normed = grad_normed.at[:, :, sources].add(spread)
        return ((update, grad_normed, grad_zero + part_zero, grad_one + part_one, grad_two + part_two), None)
    start = (jnp.zeros((25, C, ATOMS), jnp.float32), jnp.zeros((25, C, ATOMS), jnp.float32), jnp.zeros((5, C, 5 * C), jnp.float32), jnp.zeros((2, 4, C, 4 * C), jnp.float32), jnp.zeros((2, 3, C, 3 * C), jnp.float32))
    final, unused = lax.scan(shard_step, start, jnp.arange(N_GRAPH, dtype=jnp.int32))
    update, grad_normed, grad_zero, grad_one, grad_two = final
    tally = lax.optimization_barrier(jnp.sum(values * gains[:, :, None] * grad_normed, axis=(0, 1)))
    grad_embed = (inverse[None, None, :] * gains[:, :, None] * grad_normed - values * (inverse ** 3 * tally / (25 * C))[None, None, :]).astype(jnp.bfloat16)
    return (update.astype(jnp.bfloat16), grad_embed, grad_zero, grad_one, grad_two)
```

```python
import functools

import jax
import jax.numpy as jnp
from jax import lax
from jax.experimental import pallas as pl
from jax.experimental.pallas import tpu as pltpu
from jax.sharding import PartitionSpec as P


EPSILON = 1e-06
FRAME = (
    (0, 0),
    (1, 0),
    (2, 0),
    (3, 0),
    (4, 0),
    (1, 1),
    (2, 1),
    (3, 1),
    (4, 1),
    (1, -1),
    (2, -1),
    (3, -1),
    (4, -1),
    (2, 2),
    (3, 2),
    (4, 2),
    (2, -2),
    (3, -2),
    (4, -2),
)
MEMBERS = tuple(tuple(j for j, pair in enumerate(FRAME) if pair[0] == l) for l in range(5))
ROWS = (5, 8, 6)
FIRST = (0, 5, 13)
GROUP = 8
f32 = jnp.float32
bf16 = jnp.bfloat16


def degree_of(k):
    return int(k**0.5)


def full(shape):
    return pl.BlockSpec(shape, lambda *_: (0,) * len(shape))


def call(body, outs, *args, scratch=()):
    return pl.pallas_call(
        body,
        out_shape=[jax.ShapeDtypeStruct(s, d) for s, d in outs],
        scratch_shapes=list(scratch),
    )(*args)


def order_row(j):
    order = 0 if j < FIRST[1] else (1 if j < FIRST[2] else 2)
    return order, j - FIRST[order]


def one_hot(index_row, count):
    edges = index_row.shape[-1]
    rows = lax.broadcasted_iota(jnp.int32, (count, edges), 0)
    return (rows == jnp.broadcast_to(index_row, (count, edges))).astype(f32).astype(bf16)


def dot(a, b, ca=1, cb=0):
    return lax.dot_general(a, b, (((ca,), (cb,)), ((), ())), preferred_element_type=f32)


def chunk_of(local):
    return 64 if local % 64 == 0 else local


def squares_body(embed, out):
    count, local, atoms = embed.shape

    def step(k, acc):
        x = embed[k].astype(f32)
        return acc + jnp.sum((x * x).reshape(local // 8, 8, atoms), axis=0)

    acc = lax.fori_loop(0, count, step, jnp.zeros((8, atoms), f32))
    out[...] = jnp.sum(acc, axis=0, keepdims=True)


def rotate_into(source, rot, emit, local):
    cb = chunk_of(local)

    def step(i, _):
        c0 = pl.multiple_of(i * cb, cb)
        for l in range(5):
            for j in MEMBERS[l]:
                total = None
                for k in range(l * l, (l + 1) * (l + 1)):
                    term = rot[j, k : k + 1, :] * source[k, pl.ds(c0, cb), :].astype(f32)
                    total = term if total is None else total + term
                emit(j, c0, cb, total)
        return 0

    lax.fori_loop(0, local // cb, step, 0)


def grads_body(table, rot_index, target, weight, cotangent, rot, g0, g1, g2, t0, t1, t2, work):
    rots = table.shape[2]
    local = cotangent.shape[1]
    hot = one_hot(rot_index[...], rots)
    for j in range(len(FRAME)):
        value = table[j]
        high = value.astype(bf16)
        rest = value - high.astype(f32)
        middle = rest.astype(bf16)
        low = (rest - middle.astype(f32)).astype(bf16)
        rot[j] = dot(high, hot) + dot(middle, hot) + dot(low, hot)
    landing = one_hot(target[...], cotangent.shape[2])

    def gather(k, _):
        work[k] = dot(cotangent[k], landing)
        return 0

    lax.fori_loop(0, 25, gather, 0)
    grads = (g0, g1, g2)
    turned = (t0, t1, t2)
    scale = weight[...]

    def emit(j, c0, cb, total):
        order, row = order_row(j)
        grads[order][row, pl.ds(c0, cb), :] = (total * scale).astype(bf16)

    rotate_into(work, rot, emit, local)
    for j in range(len(FRAME)):
        order, row = order_row(j)
        turned[order][row] = grads[order][row].astype(f32).T.astype(bf16)


def inverse_of(squares, channels):
    return lax.rsqrt(squares / (25 * channels) + EPSILON)


def faces_body(channels, squares, gain, face, embed, out):
    inverse = inverse_of(squares[...], channels)
    hot = one_hot_rows(face[...], embed.shape[2])
    for k in range(25):
        l = degree_of(k)
        normed = (embed[k].astype(f32) * inverse * gain[:, l : l + 1]).astype(bf16)
        out[k] = dot(hot, normed, 1, 1).astype(bf16)


def one_hot_rows(index_column, count):
    rows = index_column.shape[0]
    lanes = lax.broadcasted_iota(jnp.int32, (rows, count), 1)
    return (lanes == jnp.broadcast_to(index_column, (rows, count))).astype(f32).astype(bf16)


def frame_body(channels, squares, gain, source, embed, left, right, rot, o0, o1, o2, work):
    inverse = inverse_of(squares[...], channels)
    atoms = embed.shape[2]
    local = embed.shape[1]
    halo = left.shape[1]
    hot = one_hot(source[...], atoms + 2 * halo)
    own = hot[:atoms]
    beside = hot[atoms:]
    for k in range(25):
        l = degree_of(k)
        normed = (embed[k].astype(f32) * inverse * gain[:, l : l + 1]).astype(bf16)
        faces = jnp.concatenate([left[k], right[k]], axis=0)
        work[k] = dot(normed, own) + dot(faces, beside, 0, 0)
    outs = (o0, o1, o2)

    def emit(j, c0, cb, total):
        order, row = order_row(j)
        outs[order][row, pl.ds(c0, cb), :] = total.astype(bf16)

    rotate_into(work, rot, emit, local)


def back_body(_, t0, t1, t2, w0, w1, w2, b0, b1, b2):
    step = pl.program_id(0)
    dtype = b0.dtype
    local = b0.shape[2]

    @pl.when(step < 5)
    def _():
        total = dot(t0[0], w0[0])
        for r in range(1, 5):
            total = total + dot(t0[r], w0[r])
        b0[0] = total[:, :local].astype(dtype)

    def pair(turned, weight, out, rows):
        plus = None
        for r in range(rows):
            stacked = jnp.concatenate([turned[r], turned[rows + r]], axis=0)
            real = dot(stacked, weight[0, r])
            imag = dot(stacked, weight[1, r])
            plus = real if plus is None else plus + real
            cross = imag if r == 0 else cross + imag
        edges = turned.shape[1]
        out[0, 0] = (plus[:edges] + cross[edges:])[:, :local].astype(dtype)
        out[1, 0] = (plus[edges:] - cross[:edges])[:, :local].astype(dtype)

    @pl.when((step >= 5) & (step < 9))
    def _():
        pair(t1, w1, b1, 4)

    @pl.when(step >= 9)
    def _():
        pair(t2, w2, b2, 3)


def rank_columns(weight, blocks, local, rank):
    shaped = weight.reshape(weight.shape[:-1] + (blocks, -1, local))
    mine = lax.dynamic_index_in_dim(shaped, rank, weight.ndim, keepdims=False)
    widened = jnp.pad(mine, [(0, 0)] * (mine.ndim - 1) + [(0, -local % 128)])
    return widened.reshape(weight.shape[:-1] + (-1,))


def back_part(rank, local, turned, weights, dtype):
    edges = turned[0].shape[1]
    i0 = lambda i: jnp.minimum(i, 4)
    i1 = lambda i: jnp.clip(i - 5, 0, 3)
    i2 = lambda i: jnp.clip(i - 9, 0, 2)
    ranks = weights[0].shape[-1] // (5 * local)
    if local % 128 == 0:
        weight_specs = [
            pl.BlockSpec((5, local, local), lambda i, s: (0, 0, i0(i) * ranks + s[0])),
            pl.BlockSpec((2, 4, local, local), lambda i, s: (0, 0, 0, i1(i) * ranks + s[0])),
            pl.BlockSpec((2, 3, local, local), lambda i, s: (0, 0, 0, i2(i) * ranks + s[0])),
        ]
    else:
        weights = [rank_columns(w, n, local, rank[0]) for w, n in zip(weights, (5, 4, 3))]
        weight_specs = [
            pl.BlockSpec((5, local, 128), lambda i, s: (0, 0, i0(i))),
            pl.BlockSpec((2, 4, local, 128), lambda i, s: (0, 0, 0, i1(i))),
            pl.BlockSpec((2, 3, local, 128), lambda i, s: (0, 0, 0, i2(i))),
        ]
    spec = pltpu.PrefetchScalarGridSpec(
        num_scalar_prefetch=1,
        grid=(12,),
        in_specs=[full(t.shape) for t in turned] + weight_specs,
        out_specs=[
            pl.BlockSpec((1, edges, local), lambda i, s: (i0(i), 0, 0)),
            pl.BlockSpec((2, 1, edges, local), lambda i, s: (0, i1(i), 0, 0)),
            pl.BlockSpec((2, 1, edges, local), lambda i, s: (0, i2(i), 0, 0)),
        ],
    )
    return pl.pallas_call(
        back_body,
        grid_spec=spec,
        out_shape=[
            jax.ShapeDtypeStruct((5, edges, local), dtype),
            jax.ShapeDtypeStruct((2, 4, edges, local), dtype),
            jax.ShapeDtypeStruct((2, 3, edges, local), dtype),
        ],
    )(rank, *turned, *weights)


def mix_body(f0, f1, f2, w0, w1, w2, m0, m1, m2):
    step = pl.program_id(0)

    @pl.when(step < 5)
    def _():
        m0[0] = dot(w0[0], f0[...])

    def pair(weight, frame, out):
        both = jnp.concatenate([frame[0], frame[1]], axis=1)
        real = dot(weight[0, 0], both)
        imag = dot(weight[1, 0], both)
        edges = frame.shape[2]
        out[0, 0] = real[:, :edges] - imag[:, edges:]
        out[1, 0] = real[:, edges:] + imag[:, :edges]

    @pl.when((step >= 5) & (step < 9))
    def _():
        pair(w1, f1, m1)

    @pl.when(step >= 9)
    def _():
        pair(w2, f2, m2)


def mix_forward(frames, weights):
    f0, f1, f2 = frames
    w0, w1, w2 = weights
    local = w0.shape[1]
    edges = f0.shape[-1]
    i0 = lambda i: jnp.minimum(i, 4)
    i1 = lambda i: jnp.clip(i - 5, 0, 3)
    i2 = lambda i: jnp.clip(i - 9, 0, 2)
    return pl.pallas_call(
        mix_body,
        grid=(12,),
        in_specs=[
            full(f0.shape),
            full(f1.shape),
            full(f2.shape),
            pl.BlockSpec((1, local, w0.shape[2]), lambda i: (i0(i), 0, 0)),
            pl.BlockSpec((2, 1, local, w1.shape[3]), lambda i: (0, i1(i), 0, 0)),
            pl.BlockSpec((2, 1, local, w2.shape[3]), lambda i: (0, i2(i), 0, 0)),
        ],
        out_specs=[
            pl.BlockSpec((1, local, edges), lambda i: (i0(i), 0, 0)),
            pl.BlockSpec((2, 1, local, edges), lambda i: (0, i1(i), 0, 0)),
            pl.BlockSpec((2, 1, local, edges), lambda i: (0, i2(i), 0, 0)),
        ],
        out_shape=[
            jax.ShapeDtypeStruct((5, local, edges), f32),
            jax.ShapeDtypeStruct((2, 4, local, edges), f32),
            jax.ShapeDtypeStruct((2, 3, local, edges), f32),
        ],
    )(f0, f1, f2, w0, w1, w2)


def rotate_from(fetch, rot, emit, local):
    cb = chunk_of(local)

    def step(i, _):
        c0 = pl.multiple_of(i * cb, cb)
        for l in range(5):
            values = [fetch(j, c0, cb) for j in MEMBERS[l]]
            for k in range(l * l, (l + 1) * (l + 1)):
                total = None
                for j, value in zip(MEMBERS[l], values):
                    term = rot[j, k : k + 1, :] * value
                    total = term if total is None else total + term
                emit(k, c0, cb, total)
        return 0

    lax.fori_loop(0, local // cb, step, 0)


def fetch_row(parts, j):
    order, row = order_row(j)
    if order == 0:
        return parts[0], (row,)
    half = ROWS[order] // 2
    return parts[order], (row // half, row % half)


def update_body(target, weight, rot, m0, m1, m2, out, work):
    local, atoms = out.shape[1:]
    landing = one_hot(target[...], atoms)
    scale = weight[...]

    def fetch(j, c0, cb):
        ref, at = fetch_row((m0, m1, m2), j)
        return ref[at + (pl.ds(c0, cb), slice(None))] * scale

    def emit(k, c0, cb, total):
        work[k, pl.ds(c0, cb), :] = total.astype(bf16)

    rotate_from(fetch, rot, emit, local)

    def scatter(k, _):
        out[k] = dot(work[k], landing, 1, 1).astype(bf16)
        return 0

    lax.fori_loop(0, 25, scatter, 0)


def collect_body(count, atoms, source, rot, *refs):
    parts = [refs[3 * i : 3 * i + 3] for i in range(count)]
    mine, low, high, work, spread = refs[3 * count :]
    local = mine.shape[1]
    halo = low.shape[1]
    hot = one_hot(source[...], atoms + 2 * halo)
    for j in range(len(FRAME)):
        total = None
        for part in parts:
            ref, at = fetch_row(part, j)
            value = ref[at].astype(f32)
            total = value if total is None else total + value
        work[j] = total.T

    def fetch(j, c0, cb):
        return work[j, pl.ds(c0, cb), :]

    def emit(k, c0, cb, total):
        spread[k, pl.ds(c0, cb), :] = total

    rotate_from(fetch, rot, emit, local)

    def scatter(k, _):
        value = spread[k]
        top = value.astype(bf16)
        rest = (value - top.astype(f32)).astype(bf16)
        mine[k] = dot(top, hot[:atoms], 1, 1) + dot(rest, hot[:atoms], 1, 1)
        sides = dot(hot[atoms:], top, 1, 1) + dot(hot[atoms:], rest, 1, 1)
        low[k] = sides[:halo].astype(bf16)
        high[k] = sides[halo:].astype(bf16)
        return 0

    lax.fori_loop(0, 25, scatter, 0)


def settle_body(gain, face, embed, mine, from_left, from_right, out, tally):
    atoms = embed.shape[2]
    hot = one_hot_rows(face[...], atoms)
    acc = None
    for k in range(25):
        l = degree_of(k)
        beside = jnp.concatenate([from_left[k], from_right[k]], axis=0)
        value = mine[k] + dot(beside, hot, 0, 0)
        out[k] = value
        term = embed[k].astype(f32) * gain[:, l : l + 1] * value
        acc = term if acc is None else acc + term
    tally[...] = jnp.sum(acc, axis=0, keepdims=True)


def finish_body(channels, squares, tally, gain, embed, grad, out):
    inverse = inverse_of(squares[...], channels)
    factor = inverse * inverse * inverse * tally[...] / (25 * channels)
    for k in range(25):
        l = degree_of(k)
        value = inverse * gain[:, l : l + 1] * grad[k] - embed[k].astype(f32) * factor
        out[k] = value.astype(bf16)


def lanes(ref, at, count):
    return jnp.concatenate([ref[(i,) + at] for i in range(count)], axis=1)


def weight_send_zero(members, which, grads, frame, out):
    left = lanes(frame, (which[0],), members)
    out[0] = dot(left, lanes(grads, (0,), members), 1, 1).astype(out.dtype)


def both_lanes(ref, at, members):
    plus = lanes(ref, at[0], members)
    minus = lanes(ref, at[1], members)
    return plus, minus


def weight_send_pair(members, which, grads, frame, out):
    gp, gm = both_lanes(grads, ((0, 0), (1, 0)), members)
    fp, fm = both_lanes(frame, ((which[0], 0), (which[0], 1)), members)
    out[0, 0] = (dot(fp, gp, 1, 1) + dot(fm, gm, 1, 1)).astype(out.dtype)
    out[1, 0] = (dot(fp, gm, 1, 1) - dot(fm, gp, 1, 1)).astype(out.dtype)


def weight_own_zero(members, which, grads, frame, *refs):
    out = refs[-1]
    total = dot(lanes(grads, (0,), members), lanes(frame, (which[0],), members), 1, 1)
    for part in refs[:-1]:
        total = total + part[0].astype(f32).T
    out[0] = total


def weight_own_pair(members, which, grads, frame, *refs):
    out = refs[-1]
    gp, gm = both_lanes(grads, ((0, 0), (1, 0)), members)
    fp, fm = both_lanes(frame, ((which[0], 0), (which[0], 1)), members)
    real = dot(gp, fp, 1, 1) + dot(gm, fm, 1, 1)
    imag = dot(gm, fp, 1, 1) - dot(gp, fm, 1, 1)
    for part in refs[:-1]:
        real = real + part[0, 0].astype(f32).T
        imag = imag + part[1, 0].astype(f32).T
    out[0, 0] = real
    out[1, 0] = imag


def weight_part(order, which, grads, frame, arrived, send):
    members = grads.shape[0]
    local = grads.shape[-2]
    edges = grads.shape[-1]
    width = frame.shape[-2]
    if order == 0:
        grad_spec = pl.BlockSpec((members, 1, local, edges), lambda r, s: (0, r, 0, 0))
        tall, body = (1, width, local), weight_send_zero if send else weight_own_zero
        rows = (grads.shape[1],)
        place = lambda r, s: (r, 0, 0)
    else:
        grad_spec = pl.BlockSpec((members, 2, 1, local, edges), lambda r, s: (0, 0, r, 0, 0))
        tall, body = (2, 1, width, local), weight_send_pair if send else weight_own_pair
        rows = (2, grads.shape[2])
        place = lambda r, s: (0, r, 0, 0)
    wide = tall[:-2] + (local, width)
    block, dtype = (tall, bf16) if send else (wide, f32)
    return pl.pallas_call(
        functools.partial(body, members),
        grid_spec=pltpu.PrefetchScalarGridSpec(
            num_scalar_prefetch=1,
            grid=(rows[-1],),
            in_specs=[grad_spec, full(frame.shape)] + [pl.BlockSpec(tall, place) for _ in arrived],
            out_specs=pl.BlockSpec(block, place),
        ),
        out_shape=jax.ShapeDtypeStruct(rows + block[-2:], dtype),
    )(which, grads, frame, *arrived)


def shift(axis, step):
    count = lax.axis_size(axis)
    return [(i, (i + step) % count) for i in range(count)]


def total_over(value, axis):
    total = value
    for step in range(1, lax.axis_size(axis)):
        total = total + lax.ppermute(value, axis, shift(axis, step))
    return total


def in_order(blocks, axis, dim):
    count = len(blocks)
    mine = lax.axis_index(axis)
    if count == 1:
        return blocks[0]
    if count == 2:
        first = mine == 0
        pieces = [
            jnp.where(first, blocks[0], blocks[1]),
            jnp.where(first, blocks[1], blocks[0]),
        ]
    else:
        stacked = jnp.stack(blocks)
        pieces = [
            lax.dynamic_index_in_dim(stacked, (mine - place) % count, 0, keepdims=False)
            for place in range(count)
        ]
    return jnp.concatenate(pieces, axis=dim)


def shards(
    embed,
    gain,
    w_zero,
    w_one,
    w_two,
    rot_table,
    face_atoms,
    edge_source,
    edge_target,
    rot_index,
    edge_weight,
    cotangent,
):
    _, local, atoms = embed.shape
    halo = face_atoms.shape[0] // 2
    edges = edge_source.shape[0]
    ranks = lax.axis_size("chan")
    channels = local * ranks
    devices = lax.axis_size("graph")
    group = GROUP if devices % GROUP == 0 else devices
    groups = devices // group
    rank = lax.axis_index("chan")
    here = lax.axis_index("graph")
    gains = gain.T
    source = edge_source[None, :]
    target = edge_target[None, :]
    weight = edge_weight[None, :]
    face = face_atoms[:, None]
    weights = (w_zero, w_one, w_two)

    squares = call(squares_body, [((1, atoms), f32)], embed)[0]
    squares = total_over(squares, "chan")

    shapes = [((n, local, edges), bf16) for n in ROWS]
    turned_shapes = [((n, edges, local), bf16) for n in ROWS]
    rot, g0, g1, g2, *turned = call(
        grads_body,
        [((len(FRAME), 25, edges), f32)] + shapes + turned_shapes,
        rot_table,
        rot_index[None, :],
        target,
        weight,
        cotangent,
        scratch=[pltpu.VMEM((25, local, edges), f32)],
    )
    g1 = g1.reshape(2, 4, local, edges)
    g2 = g2.reshape(2, 3, local, edges)
    teams = [[h * group + i for i in range(group)] for h in range(groups)]
    gathered = [
        lax.all_gather(g, "graph", axis_index_groups=teams if groups > 1 else None)
        for g in (g0, g1, g2)
    ]

    faces = call(
        functools.partial(faces_body, channels),
        [((25, 2 * halo, local), bf16)],
        squares,
        gains,
        face,
        embed,
    )[0]
    left = lax.ppermute(faces[:, halo:], "graph", shift("graph", 1))
    right = lax.ppermute(faces[:, :halo], "graph", shift("graph", -1))
    owns = call(
        functools.partial(frame_body, channels),
        shapes,
        squares,
        gains,
        source,
        embed,
        left,
        right,
        rot,
        scratch=[pltpu.VMEM((25, local, edges), f32)],
    )
    frames = []
    for own, split in zip(owns, (1, 2, 2)):
        blocks = [own] + [
            lax.ppermute(own, "chan", shift("chan", step)) for step in range(1, ranks)
        ]
        whole = in_order(blocks, "chan", 1)
        frames.append(whole.reshape(split, -1, edges))

    sent = []
    for step in range(1, ranks):
        to = ((rank + step) % ranks).astype(jnp.int32)[None]
        parts = back_part(to, local, turned, weights, bf16)
        sent.append([lax.ppermute(part, "chan", shift("chan", step)) for part in parts])
    backs = [back_part(rank.astype(jnp.int32)[None], local, turned, weights, f32)] + sent

    mine, low, high = call(
        functools.partial(collect_body, len(backs), atoms),
        [((25, local, atoms), f32), ((25, halo, local), bf16), ((25, halo, local), bf16)],
        source,
        rot,
        *[part for parts in backs for part in parts],
        scratch=[
            pltpu.VMEM((len(FRAME), local, edges), f32),
            pltpu.VMEM((25, local, edges), f32),
        ],
    )
    from_left = lax.ppermute(high, "graph", shift("graph", 1))
    from_right = lax.ppermute(low, "graph", shift("graph", -1))
    grad, tally = call(
        settle_body,
        [((25, local, atoms), f32), ((1, atoms), f32)],
        gains,
        face,
        embed,
        mine,
        from_left,
        from_right,
    )
    tally = total_over(tally, "chan")
    grad_embed = call(
        functools.partial(finish_body, channels),
        [((25, local, atoms), bf16)],
        squares,
        tally,
        gains,
        embed,
        grad,
    )[0]

    mixed = mix_forward((frames[0][0], frames[1], frames[2]), weights)
    update = call(
        update_body,
        [((25, local, atoms), bf16)],
        target,
        weight,
        rot,
        *mixed,
        scratch=[pltpu.VMEM((25, local, edges), bf16)],
    )[0]

    home = here // group
    results = []
    for order in (2, 1, 0):
        frame = frames[order]
        pairs, rows = frame.shape[:2]
        width = rows // devices
        cut = frame.reshape(pairs, groups, group, width, edges).transpose(2, 1, 0, 3, 4)
        if group > 1:
            cut = lax.all_to_all(
                cut, "graph", 0, 0, axis_index_groups=teams if groups > 1 else None
            )
        if order == 0:
            cut = cut[:, :, 0]
        arrived = []
        for step in range(1, groups):
            other = ((home + step) % groups).astype(jnp.int32)[None]
            part = weight_part(order, other, gathered[order], cut, (), True)
            arrived.append(lax.ppermute(part, "graph", shift("graph", step * group)))
        results.append(
            weight_part(order, home.astype(jnp.int32)[None], gathered[order], cut, arrived, False)
        )
    grad_two, grad_one, grad_zero = results
    return (update, grad_embed, grad_zero, grad_one, grad_two)


def solution(mesh):
    placed = (
        P(None, "chan", "graph"),
        P(None, "chan"),
        P(None, "chan", None),
        P(None, None, "chan", None),
        P(None, None, "chan", None),
        P(),
        P("graph"),
        P("graph"),
        P("graph"),
        P("graph"),
        P("graph"),
        P(None, "chan", "graph"),
    )
    return jax.shard_map(
        shards,
        mesh=mesh,
        in_specs=placed,
        out_specs=(
            P(None, "chan", "graph"),
            P(None, "chan", "graph"),
            P(None, "chan", "graph"),
            P(None, None, "chan", "graph"),
            P(None, None, "chan", "graph"),
        ),
        check_vma=False,
    )
```

```python
import functools

import jax
import jax.numpy as jnp
from jax import lax
from jax.experimental import pallas as pl
from jax.experimental.pallas import tpu as pltpu
from jax.sharding import PartitionSpec as P


EPSILON = 1e-06
FRAME = (
    (0, 0),
    (1, 0),
    (2, 0),
    (3, 0),
    (4, 0),
    (1, 1),
    (2, 1),
    (3, 1),
    (4, 1),
    (1, -1),
    (2, -1),
    (3, -1),
    (4, -1),
    (2, 2),
    (3, 2),
    (4, 2),
    (2, -2),
    (3, -2),
    (4, -2),
)
MEMBERS = tuple(tuple(j for j, pair in enumerate(FRAME) if pair[0] == l) for l in range(5))
GROUP = 8
RATE = 4000000
VMEM = 56 * 1024 * 1024
f32 = jnp.float32
bf16 = jnp.bfloat16


def degree_of(k):
    return int(k**0.5)


def full(shape):
    return pl.BlockSpec(shape, lambda *_: (0,) * len(shape))


def call(body, outs, *args, scratch=(), us=1, hold=(), scalars=0):
    memory = lambda i: pl.ANY if i in hold else (pltpu.SMEM if i < scalars else pltpu.VMEM)
    return pl.pallas_call(
        body,
        in_specs=[pl.BlockSpec(memory_space=memory(i)) for i in range(len(args))],
        out_shape=[jax.ShapeDtypeStruct(s, d) for s, d in outs],
        scratch_shapes=list(scratch),
        name=getattr(body, "func", body).__name__,
        cost_estimate=pl.CostEstimate(flops=int(us * RATE), bytes_accessed=0, transcendentals=0),
        compiler_params=pltpu.CompilerParams(vmem_limit_bytes=VMEM),
    )(*args)


def piece_row(j):
    if j < 5:
        return 1, j
    return (0, j - 5) if j < 13 else (1, j - 8)


def one_hot(index_row, count):
    edges = index_row.shape[-1]
    rows = lax.broadcasted_iota(jnp.int32, (count, edges), 0)
    return (rows == jnp.broadcast_to(index_row, (count, edges))).astype(f32).astype(bf16)


def one_hot_rows(index_column, count):
    rows = index_column.shape[0]
    lanes = lax.broadcasted_iota(jnp.int32, (rows, count), 1)
    return (lanes == jnp.broadcast_to(index_column, (rows, count))).astype(f32).astype(bf16)


def dot(a, b, ca=1, cb=0):
    return lax.dot_general(a, b, (((ca,), (cb,)), ((), ())), preferred_element_type=f32)


def chunk_of(local):
    return 64 if local % 64 == 0 else local


def fold(x):
    return jnp.sum(x.reshape(-1, 32, x.shape[-1]), axis=0)


def first_body(face, embed, squares, raw):
    atoms = embed.shape[2]
    hot = one_hot_rows(face[...], atoms)
    acc = None
    for k in range(25):
        x = embed[k].astype(f32)
        term = fold(x * x)
        acc = term if acc is None else acc + term
        raw[k] = dot(hot, embed[k], 1, 1).astype(bf16)
    squares[...] = jnp.sum(acc, axis=0, keepdims=True)


def beside_body(left, right, out):
    for i, side in enumerate((left, right)):
        acc = None
        for k in range(25):
            x = side[k].astype(f32)
            acc = x * x if acc is None else acc + x * x
        out[i] = jnp.sum(acc, axis=1, keepdims=True)


def rotate_into(source, rot, emit, local):
    cb = chunk_of(local)

    def step(i, _):
        c0 = pl.multiple_of(i * cb, cb)
        for l in range(5):
            for j in MEMBERS[l]:
                total = None
                for k in range(l * l, (l + 1) * (l + 1)):
                    term = rot[k, j : j + 1, :] * source[k, pl.ds(c0, cb), :].astype(f32)
                    total = term if total is None else total + term
                emit(j, c0, cb, total)
        return 0

    lax.fori_loop(0, local // cb, step, 0)


def rotate_from(fetch, rot, emit, local):
    cb = chunk_of(local)

    def step(i, _):
        c0 = pl.multiple_of(i * cb, cb)
        for l in range(5):
            values = [fetch(j, c0, cb) for j in MEMBERS[l]]
            for k in range(l * l, (l + 1) * (l + 1)):
                total = None
                for j, value in zip(MEMBERS[l], values):
                    term = rot[k, j : j + 1, :] * value
                    total = term if total is None else total + term
                emit(k, c0, cb, total)
        return 0

    lax.fori_loop(0, local // cb, step, 0)


def grads_body(table, rot_index, target, weight, cotangent, rot, ga, gb, turned, work):
    rots = table.shape[2]
    count, local, atoms = cotangent.shape
    hot = one_hot(rot_index[...], rots)
    for k in range(count):
        value = table[k]
        high = value.astype(bf16)
        rest = value - high.astype(f32)
        middle = rest.astype(bf16)
        low = (rest - middle.astype(f32)).astype(bf16)
        rot[k] = dot(high, hot) + dot(middle, hot) + dot(low, hot)
    landing = one_hot(target[...], atoms)
    edges = landing.shape[1]
    found = dot(cotangent[...].reshape(count * local, atoms), landing)
    work[...] = found.reshape(count, local, edges)
    grads = (ga, gb)
    scale = weight[...]

    def emit(j, c0, cb, total):
        piece, row = piece_row(j)
        grads[piece][row, pl.ds(c0, cb), :] = (total * scale).astype(bf16)

    rotate_into(work, rot, emit, local)
    for j in range(len(FRAME)):
        piece, row = piece_row(j)
        turned[j] = grads[piece][row].astype(f32).T.astype(bf16)


def inverse_of(squares, channels):
    return lax.rsqrt(squares / (25 * channels) + EPSILON)


def frame_body(channels, squares, aside, gain, gain_t, source, embed, left, right, rot, fa, fb, work):
    inverse = inverse_of(squares[...], channels)
    outer = inverse_of(jnp.concatenate([aside[0], aside[1]], axis=0), channels)
    count, local, atoms = embed.shape
    halo = left.shape[1]
    hot = one_hot(source[...], atoms + 2 * halo)
    own = hot[:atoms]
    beside = hot[atoms:]
    for k in range(count):
        l = degree_of(k)
        normed = (embed[k].astype(f32) * inverse * gain_t[:, l : l + 1]).astype(bf16)
        faces = jnp.concatenate([left[k], right[k]], axis=0).astype(f32)
        faces = (faces * outer * gain[l : l + 1, :]).astype(bf16)
        work[k] = dot(normed, own) + dot(faces, beside, 0, 0)
    outs = (fa, fb)

    def emit(j, c0, cb, total):
        piece, row = piece_row(j)
        outs[piece][row, pl.ds(c0, cb), :] = total.astype(bf16)

    rotate_into(work, rot, emit, local)


def join_body(groups, splits, rank, *refs):
    *blocks, whole, cut = refs
    count = len(blocks)
    rows, local, _ = blocks[0].shape
    channels = count * local
    for i, block in enumerate(blocks):
        at = (rank[0] + count - i) % count * local
        for r in range(rows):
            start = pl.multiple_of(at + r * channels, local)
            whole[pl.ds(start, local), :] = block[r]
    members = cut.shape[0]
    base = 0
    below = 0
    for blocks_here, copies in splits:
        size = blocks_here * channels
        width = size // (members * groups)
        for copy in range(copies):
            for q in range(members * groups):
                start = base + q * width
                cut[q % members, q // members, below : below + width] = whole[start : start + width]
            base += size
            below += width


def joined(blocks, splits, rank, members, groups):
    rows, local, edges = blocks[0].shape
    height = rows * local * len(blocks)
    return call(
        functools.partial(join_body, groups, splits),
        [((height, edges), bf16), ((members, groups, height // (members * groups), edges), bf16)],
        rank,
        *blocks,
        us=2,
        scalars=1,
    )


def load_all(pairs, sems):
    copies = []
    for source, target in pairs:
        copies.append(pltpu.make_async_copy(source, target, sems.at[len(copies)]))
    for copy in copies:
        copy.start()
    return copies


def weight_pairs(weights, buffers):
    pairs = [(weights[0].at[r], buffers[0].at[r]) for r in range(5)]
    pairs += [(weights[1].at[i, r], buffers[1].at[i, r]) for i in range(2) for r in range(4)]
    pairs += [(weights[2].at[i, r], buffers[2].at[i, r]) for i in range(2) for r in range(3)]
    return pairs


def turned_dot(parts, weight):
    local = parts[0].shape[1]
    if local % 128 == 0:
        return dot(jnp.concatenate(parts, axis=1), weight.reshape(-1, weight.shape[-1]))
    total = dot(parts[0], weight[0])
    for r in range(1, len(parts)):
        total = total + dot(parts[r], weight[r])
    return total


def back_body(rank, turned, w0, w1, w2, out, v0, v1, v2, sems):
    copies = load_all(weight_pairs((w0, w1, w2), (v0, v1, v2)), sems)
    count, _, edges, local = out.shape

    def put(row, value, blocks):
        for s in range(blocks):
            for h in range(count):
                slot = (h + count - rank[0]) % count
                at = (s * count + h) * local
                out[slot, row + s] = value[:, at : at + local].astype(bf16)

    for copy in copies[:5]:
        copy.wait()
    put(0, turned_dot([turned[j] for j in range(5)], v0[...]), 5)
    for first, blocks, buffer, waits in ((5, 4, v1, copies[5:13]), (13, 3, v2, copies[13:])):
        for copy in waits:
            copy.wait()
        parts = [
            jnp.concatenate([turned[first + r], turned[first + blocks + r]], axis=0)
            for r in range(blocks)
        ]
        real = turned_dot(parts, buffer[0])
        imag = turned_dot(parts, buffer[1])
        put(first, real[:edges] + imag[edges:], blocks)
        put(first + blocks, real[edges:] - imag[:edges], blocks)


def weight_scratch(weights):
    return [pltpu.VMEM(w.shape, w.dtype) for w in weights] + [pltpu.SemaphoreType.DMA((19,))]


def update_body(target, weight, rot, fa, fb, w0, w1, w2, out, v0, v1, v2, sems, mixed, work):
    copies = load_all(weight_pairs((w0, w1, w2), (v0, v1, v2)), sems)
    count, local, atoms = out.shape
    edges = fa.shape[1]
    scale = weight[...]
    span0, span1, span2 = w0.shape[-1], w1.shape[-1], w2.shape[-1]
    for copy in copies[:5]:
        copy.wait()
    mixed[0:5] = dot(v0[...].reshape(-1, span0), fb[0:span0]).reshape(5, local, edges)
    for first, blocks, buffer, waits, frame, base, span in (
        (5, 4, v1, copies[5:13], fa, 0, span1),
        (13, 3, v2, copies[13:], fb, span0, span2),
    ):
        for copy in waits:
            copy.wait()
        both = jnp.concatenate([frame[base : base + span], frame[base + span : base + 2 * span]], axis=1)
        real = dot(buffer[0].reshape(-1, span), both)
        imag = dot(buffer[1].reshape(-1, span), both)
        plus = real[:, :edges] - imag[:, edges:]
        minus = real[:, edges:] + imag[:, :edges]
        mixed[first : first + blocks] = plus.reshape(blocks, local, edges)
        mixed[first + blocks : first + 2 * blocks] = minus.reshape(blocks, local, edges)
    landing = one_hot(target[...], atoms)

    def fetch(j, c0, cb):
        return mixed[j, pl.ds(c0, cb), :] * scale

    def emit(k, c0, cb, total):
        work[k, pl.ds(c0, cb), :] = total.astype(bf16)

    rotate_from(fetch, rot, emit, local)
    landed = dot(work[...].reshape(count * local, edges), landing, 1, 1)
    out[...] = landed.astype(bf16).reshape(count, local, atoms)


def collect_body(atoms, source, rot, *refs):
    *parts, mine, low, high, work, spread = refs
    count, local, _ = mine.shape
    edges = rot.shape[2]
    halo = low.shape[1]
    hot = one_hot(source[...], atoms + 2 * halo)
    for j in range(len(FRAME)):
        total = None
        for part in parts:
            value = part[0, j].astype(f32)
            total = value if total is None else total + value
        work[j] = total.T

    def fetch(j, c0, cb):
        return work[j, pl.ds(c0, cb), :]

    def emit(k, c0, cb, total):
        top = total.astype(bf16)
        spread[k, pl.ds(c0, cb), :edges] = top
        spread[k, pl.ds(c0, cb), edges:] = (total - top.astype(f32)).astype(bf16)

    rotate_from(fetch, rot, emit, local)
    twice = jnp.concatenate([hot, hot], axis=1)
    split = spread[...].reshape(count * local, 2 * edges)
    mine[...] = dot(split, twice[:atoms], 1, 1).reshape(count, local, atoms)
    for k in range(count):
        sides = dot(twice[atoms:], spread[k], 1, 1)
        low[k] = sides[:halo].astype(bf16)
        high[k] = sides[halo:].astype(bf16)


def settled(k, mine, from_left, from_right, hot):
    beside = jnp.concatenate([from_left[k], from_right[k]], axis=0)
    return mine[k] + dot(beside, hot, 0, 0)


def settle_body(gain, face, embed, mine, from_left, from_right, tally):
    hot = one_hot_rows(face[...], embed.shape[2])
    acc = None
    for k in range(25):
        l = degree_of(k)
        value = settled(k, mine, from_left, from_right, hot)
        term = fold(embed[k].astype(f32) * gain[:, l : l + 1] * value)
        acc = term if acc is None else acc + term
    tally[...] = jnp.sum(acc, axis=0, keepdims=True)


def finish_body(channels, squares, tally, gain, face, embed, mine, from_left, from_right, out):
    hot = one_hot_rows(face[...], embed.shape[2])
    inverse = inverse_of(squares[...], channels)
    factor = inverse * inverse * inverse * tally[...] / (25 * channels)
    for k in range(25):
        l = degree_of(k)
        grad = settled(k, mine, from_left, from_right, hot)
        value = inverse * gain[:, l : l + 1] * grad - embed[k].astype(f32) * factor
        out[k] = value.astype(bf16)


def lanes(parts):
    return jnp.concatenate(parts, axis=1)


def turned_out(width):
    return width % 128 != 0


def weight_rows(splits):
    rows = []
    base = 0
    for blocks, copies in splits:
        rows.append((base, blocks, copies))
        base += blocks * copies
    return rows


def weight_body(splits, which, grads, frame, *refs):
    arrived = refs[: len(refs) - len(splits) - 2]
    outs = refs[len(arrived) : len(refs) - 2]
    buffer, sems = refs[-2:]
    members = frame.shape[0]
    devices = members * frame.shape[1]
    local = grads.shape[2]
    h = which[0]
    total = buffer.shape[1]
    copies = load_all([(grads.at[:, r], buffer.at[:, r]) for r in range(total)], sems)

    def left(row):
        return lanes([buffer[i, row] for i in range(members)])

    def right(at, width):
        return lanes([frame[i, h, at : at + width] for i in range(members)])

    below = 0
    for index, (base, blocks, copy) in enumerate(weight_rows(splits)):
        out = outs[index]
        turned = out.shape[-1] == local and out.shape[-2] != local
        width = out.shape[-2] if turned else out.shape[-1]
        mul = (lambda g, f: dot(f, g, 1, 1)) if turned else (lambda g, f: dot(g, f, 1, 1))
        fp = right(below, width)
        if copy == 2:
            fm = right(below + width, width)
            both = lanes([fp, fm])
            cross = lanes([-fm, fp])
        for r in range(blocks):
            copies[base + r].wait()
            if copy == 1:
                values = [mul(left(base + r), fp)]
                places = [(r,)]
            else:
                copies[base + blocks + r].wait()
                g = lanes([left(base + r), left(base + blocks + r)])
                values = [mul(g, both), mul(g, cross)]
                places = [(0, r), (1, r)]
            for value, place in zip(values, places):
                for part in arrived[index :: len(splits)]:
                    value = value + part[place].astype(f32)
                out[place] = value.astype(out.dtype)
        below += width * copy


def weight_part(splits, which, grads, frame, arrived, devices, dtype):
    members, rows, local, edges = grads.shape
    channels = frame.shape[2] * devices // rows
    outs = []
    for blocks, copies in splits:
        width = blocks * channels // devices
        tile = (width, local) if turned_out(width) and width != local else (local, width)
        outs.append((((2,) if copies == 2 else ()) + (blocks,) + tile, dtype))
    return call(
        functools.partial(weight_body, splits),
        outs,
        which,
        grads,
        frame,
        *arrived,
        scratch=[pltpu.VMEM(grads.shape, bf16), pltpu.SemaphoreType.DMA((rows,))],
        us=3,
        hold=(1,),
        scalars=1,
    )


def shift(axis, step):
    count = lax.axis_size(axis)
    return [(i, (i + step) % count) for i in range(count)]


def total_over(value, axis):
    total = value
    for step in range(1, lax.axis_size(axis)):
        total = total + lax.ppermute(value, axis, shift(axis, step))
    return total


def shards(
    embed,
    gain,
    w_zero,
    w_one,
    w_two,
    rot_table,
    face_atoms,
    edge_source,
    edge_target,
    rot_index,
    edge_weight,
    cotangent,
):
    _, local, atoms = embed.shape
    halo = face_atoms.shape[0] // 2
    edges = edge_source.shape[0]
    ranks = lax.axis_size("chan")
    channels = local * ranks
    devices = lax.axis_size("graph")
    group = GROUP if devices % GROUP == 0 else devices
    groups = devices // group
    teams = [[h * group + i for i in range(group)] for h in range(groups)] if groups > 1 else None
    rank = lax.axis_index("chan").astype(jnp.int32)[None]
    home = lax.axis_index("graph") // group
    gain_t = gain.T
    source = edge_source[None, :]
    target = edge_target[None, :]
    weight = edge_weight[None, :]
    face = face_atoms[:, None]
    weights = (w_zero, w_one, w_two)
    frames_f32 = pltpu.VMEM((25, local, edges), f32)

    squares, raw = call(
        first_body, [((1, atoms), f32), ((25, 2 * halo, local), bf16)], face, embed, us=3
    )
    left = lax.ppermute(raw[:, halo:], "graph", shift("graph", 1))
    right = lax.ppermute(raw[:, :halo], "graph", shift("graph", -1))
    rot, ga, gb, turned = call(
        grads_body,
        [
            ((25, len(FRAME), edges), f32),
            ((8, local, edges), bf16),
            ((11, local, edges), bf16),
            ((len(FRAME), edges, local), bf16),
        ],
        rot_table.transpose(1, 0, 2),
        rot_index[None, :],
        target,
        weight,
        cotangent,
        scratch=[frames_f32],
        us=7,
    )
    gathered = [lax.all_gather(g, "graph", axis_index_groups=teams) for g in (ga, gb)]
    aside = call(beside_body, [((2, halo, 1), f32)], left, right, us=1)[0]
    both = jnp.concatenate([squares[0], aside.reshape(-1)])
    both = total_over(both, "chan")
    squares = both[:atoms][None, :]
    aside = both[atoms:].reshape(2, halo, 1)
    owns = call(
        functools.partial(frame_body, channels),
        [((8, local, edges), bf16), ((11, local, edges), bf16)],
        squares,
        aside,
        gain,
        gain_t,
        source,
        embed,
        left,
        right,
        rot,
        scratch=[frames_f32],
        us=5,
    )
    splits = (((4, 2),), ((5, 1), (3, 2)))
    frames, cuts = [], []
    for own, split in zip(owns, splits):
        blocks = [own] + [
            lax.ppermute(own, "chan", shift("chan", step)) for step in range(1, ranks)
        ]
        whole, cut = joined(blocks, split, rank, group, groups)
        frames.append(whole)
        cuts.append(lax.all_to_all(cut, "graph", 0, 0, axis_index_groups=teams))

    backs = call(
        back_body,
        [((ranks, len(FRAME), edges, local), bf16)],
        rank,
        turned,
        *weights,
        scratch=weight_scratch(weights),
        us=9,
        hold=(2, 3, 4),
        scalars=1,
    )[0]
    parts = [backs[:1]] + [
        lax.ppermute(backs[step : step + 1], "chan", shift("chan", step))
        for step in range(1, ranks)
    ]

    sent = []
    for piece, split in enumerate(splits):
        arrived = []
        for step in range(1, groups):
            other = ((home + step) % groups).astype(jnp.int32)[None]
            outs = weight_part(split, other, gathered[piece], cuts[piece], (), devices, bf16)
            arrived += [
                lax.ppermute(out, "graph", shift("graph", step * group)) for out in outs
            ]
        sent.append(arrived)

    update = call(
        update_body,
        [((25, local, atoms), bf16)],
        target,
        weight,
        rot,
        *frames,
        *weights,
        scratch=weight_scratch(weights)
        + [pltpu.VMEM((len(FRAME), local, edges), f32), pltpu.VMEM((25, local, edges), bf16)],
        us=15,
        hold=(5, 6, 7),
    )[0]

    mine, low, high = call(
        functools.partial(collect_body, atoms),
        [((25, local, atoms), f32), ((25, halo, local), bf16), ((25, halo, local), bf16)],
        source,
        rot,
        *parts,
        scratch=[
            pltpu.VMEM((len(FRAME), local, edges), f32),
            pltpu.VMEM((25, local, 2 * edges), bf16),
        ],
        us=8,
    )
    from_left = lax.ppermute(high, "graph", shift("graph", 1))
    from_right = lax.ppermute(low, "graph", shift("graph", -1))
    tally = call(
        settle_body,
        [((1, atoms), f32)],
        gain_t,
        face,
        embed,
        mine,
        from_left,
        from_right,
        us=4,
    )[0]
    tally = total_over(tally, "chan")
    grad_embed = call(
        functools.partial(finish_body, channels),
        [((25, local, atoms), bf16)],
        squares,
        tally,
        gain_t,
        face,
        embed,
        mine,
        from_left,
        from_right,
        us=4,
    )[0]

    mixing = []
    for piece, split in enumerate(splits):
        outs = weight_part(
            split, home.astype(jnp.int32)[None], gathered[piece], cuts[piece], sent[piece], devices, f32
        )
        for out, (blocks, _) in zip(outs, split):
            width = blocks * channels // devices
            mixing.append(out if out.shape[-2:] == (local, width) else jnp.swapaxes(out, -1, -2))
    grad_one, grad_zero, grad_two = mixing
    return (update, grad_embed, grad_zero, grad_one, grad_two)


def solution(mesh):
    placed = (
        P(None, "chan", "graph"),
        P(None, "chan"),
        P(None, "chan", None),
        P(None, None, "chan", None),
        P(None, None, "chan", None),
        P(),
        P("graph"),
        P("graph"),
        P("graph"),
        P("graph"),
        P("graph"),
        P(None, "chan", "graph"),
    )
    return jax.shard_map(
        shards,
        mesh=mesh,
        in_specs=placed,
        out_specs=(
            P(None, "chan", "graph"),
            P(None, "chan", "graph"),
            P(None, "chan", "graph"),
            P(None, None, "chan", "graph"),
            P(None, None, "chan", "graph"),
        ),
        check_vma=False,
    )
```
